16 devices in a mesh: tp: 16 (over z, y, x, core).
Axes of the slice: x: 2, y: 2, z: 2, core: 2. Of those that a mesh axis runs over, the one named last changes fastest.
Arguments:
- hidden: bfloat16 [4, 8192, 1024], P(None, 'tp')
- labels: int32 [4, 8192], P(None, 'tp')
- loss_mask: int32 [4, 8192], P(None, 'tp')
- norm_gain: float32 [1024], replicated
- w_head: bfloat16 [1024, 32768], P(None, 'tp')
Outputs:
- output 1: float32 [], replicated
- output 2: bfloat16 [4, 8192, 1024], P(None, 'tp')
- output 3: bfloat16 [1024, 32768], P(None, 'tp')
- output 4: float32 [1024], replicated
All inputs are finite; a program needn't handle non-finite values.
Results may differ from the reference program's by a relative error of at most 0.0086346.
Values are sent between devices in bfloat16 or wider.
A program may use at most 1 GiB of HBM per device.

```python
import jax
import jax.numpy as jnp
from jax import lax

BATCH_SIZE = 4
SEQ_DEV = 512
D_MODEL = 1024
VOCAB_SIZE = 32768
SHARDS = 16
SEQ_LEN = SEQ_DEV * SHARDS
VSHARD = VOCAB_SIZE // SHARDS
NORM_EPS = 1e-6
LOGIT_STD = 3.0
LABEL_PULL = 2.0


def draw_targets(route_key):
    key_hot, key_pick, key_uni, key_loc, key_rate, key_keep = jax.random.split(route_key, 6)
    hot_block = jax.random.randint(key_hot, (), 0, SHARDS)
    use_hot = jax.random.randint(key_pick, (BATCH_SIZE, SEQ_LEN), 0, 2)
    spread_ids = jax.random.randint(key_uni, (BATCH_SIZE, SEQ_LEN), 0, VOCAB_SIZE)
    hot_ids = hot_block * VSHARD + jax.random.randint(key_loc, (BATCH_SIZE, SEQ_LEN), 0, VSHARD)
    labels = jnp.where(use_hot == 1, hot_ids, spread_ids).astype(jnp.int32)
    keep_rate = jax.random.randint(key_rate, (BATCH_SIZE, SHARDS, 1), 1, 9)
    keep_draw = jax.random.randint(key_keep, (BATCH_SIZE, SHARDS, SEQ_DEV), 0, 8)
    loss_mask = (keep_draw < keep_rate).astype(jnp.int32).reshape(BATCH_SIZE, SEQ_LEN)
    first_pos = (jnp.arange(SEQ_LEN) == 0).astype(jnp.int32)
    loss_mask = jnp.maximum(loss_mask, first_pos[None, :])
    return labels, loss_mask


def setup_inputs(seed: int = 0) -> dict:
    root_key = jax.random.key(seed)
    key_route, key_head, key_noise, key_row, key_gain = jax.random.split(root_key, 5)
    labels, loss_mask = draw_targets(key_route)
    w_f32 = jax.random.normal(key_head, (D_MODEL, VOCAB_SIZE), jnp.float32) * (LOGIT_STD * D_MODEL ** -0.5)
    label_dirs = jnp.moveaxis(jnp.take(w_f32, labels, axis=1), 0, -1) * (D_MODEL ** 0.5 / LOGIT_STD)
    noise = jax.random.normal(key_noise, (BATCH_SIZE, SEQ_LEN, D_MODEL), jnp.float32)
    row_scale = jax.random.uniform(key_row, (BATCH_SIZE, SEQ_LEN, 1), jnp.float32, 0.5, 2.0)
    hidden = (row_scale * (noise + LABEL_PULL * D_MODEL ** -0.5 * label_dirs)).astype(jnp.bfloat16)
    norm_gain = 1.0 + 0.4 * jax.random.normal(key_gain, (D_MODEL,), jnp.float32)
    return {'hidden': hidden, 'labels': labels, 'loss_mask': loss_mask, 'norm_gain': norm_gain, 'w_head': w_f32.astype(jnp.bfloat16)}


def rms_norm(x_rows, norm_gain):
    inv_rms = lax.rsqrt(jnp.mean(x_rows * x_rows, axis=-1, keepdims=True) + NORM_EPS)
    return x_rows * inv_rms * norm_gain


def reference(hidden, labels, loss_mask, norm_gain, w_head):
    tokens = BATCH_SIZE * SEQ_LEN
    n_blocks = tokens // SEQ_DEV
    x_rows = hidden.reshape(tokens, D_MODEL).astype(jnp.float32)
    norm_out, norm_vjp = jax.vjp(rms_norm, x_rows, norm_gain)
    hn_rows = norm_out.astype(jnp.bfloat16)
    hn_cols = hn_rows.T
    label_ids = labels.reshape(tokens)
    tok_weight = loss_mask.reshape(tokens).astype(jnp.float32)
    kept_count = jnp.sum(tok_weight)

    def token_stats(blk_pair):
        hn_blk, lab_blk = blk_pair
        logits = jnp.dot(hn_blk, w_head, preferred_element_type=jnp.float32)
        row_max = jnp.max(logits, axis=-1)
        blk_norm = row_max + jnp.log(jnp.sum(jnp.exp(logits - row_max[:, None]), axis=-1))
        blk_label = jnp.take_along_axis(logits, lab_blk[:, None], axis=-1)[:, 0]
        return blk_norm, blk_label

    log_norm, label_logit = lax.map(token_stats, (hn_rows.reshape(n_blocks, SEQ_DEV, D_MODEL), label_ids.reshape(n_blocks, SEQ_DEV)))
    log_norm = log_norm.reshape(tokens)
    label_logit = label_logit.reshape(tokens)
    mean_loss = jnp.sum(tok_weight * (log_norm - label_logit)) / kept_count
    tok_scale = tok_weight / kept_count
    w_blocks = jnp.transpose(w_head.reshape(D_MODEL, SHARDS, VSHARD), (1, 0, 2))

    def shard_step(d_norm, shard_in):
        w_blk, shard_idx = shard_in
        logits = jnp.dot(hn_rows, w_blk, preferred_element_type=jnp.float32)
        col_ids = shard_idx * VSHARD + jnp.arange(VSHARD)
        is_label = (label_ids[:, None] == col_ids[None, :]).astype(jnp.float32)
        d_logits = ((jnp.exp(logits - log_norm[:, None]) - is_label) * tok_scale[:, None]).astype(jnp.bfloat16)
        d_blk = jnp.dot(hn_cols, d_logits, preferred_element_type=jnp.float32).astype(jnp.bfloat16)
        dhn_part = jnp.dot(d_logits, w_blk.T, preferred_element_type=jnp.float32).astype(jnp.bfloat16)
        return d_norm + dhn_part.astype(jnp.float32), d_blk

    d_norm, d_blocks = lax.scan(shard_step, jnp.zeros((tokens, D_MODEL), jnp.float32), (w_blocks, jnp.arange(SHARDS)))
    d_head = jnp.transpose(d_blocks, (1, 0, 2)).reshape(D_MODEL, VOCAB_SIZE)
    d_x, d_gain = norm_vjp(d_norm)
    d_hidden = d_x.astype(jnp.bfloat16).reshape(BATCH_SIZE, SEQ_LEN, D_MODEL)
    return mean_loss, d_hidden, d_head, d_gain
```

```python
import functools

import jax
import jax.numpy as jnp
from jax import lax
from jax.experimental import pallas as pl
from jax.experimental.pallas import tpu as pltpu
from jax.sharding import PartitionSpec as P


NORM_EPS = 1e-6

CORE, X, Y, Z = 1, 2, 4, 8
TM1 = 256
TM2 = 512
NC = 512
LANES = 128
ROWS = 8


def rms_norm(x_rows, norm_gain):
    inv_rms = lax.rsqrt(jnp.mean(x_rows * x_rows, axis=-1, keepdims=True) + NORM_EPS)
    return x_rows * inv_rms * norm_gain


def columns_of(rows_ref):
    rows = rows_ref[...]
    return jnp.concatenate([rows, jnp.zeros((LANES - ROWS, rows.shape[1]), rows.dtype)]).T


def logits_kernel(parts, lane0, copy_hn, n_prev, *refs):
    rows_ref = refs[0]
    a_refs = refs[1:1 + len(parts)]
    w_refs = refs[1 + len(parts):3 + len(parts)]
    outs = refs[3 + len(parts) + n_prev:]
    z_ref, st_ref = outs[0], outs[1]
    if copy_hn:
        hn_ref = outs[2]
        i = pl.program_id(0)
        for a_ref, (lo, hi) in zip(a_refs, parts):
            @pl.when((i >= lo) & (i < hi))
            def _(a_ref=a_ref):
                hn_ref[...] = a_ref[...]
        a = hn_ref[...]
    else:
        a = a_refs[0][...]
    tm = a.shape[0]
    rows = columns_of(rows_ref)
    lane = lax.broadcasted_iota(jnp.int32, (tm, LANES), 1)
    lane_f = lane.astype(jnp.float32)
    m = jnp.full((tm, LANES), -jnp.inf, jnp.float32)
    s = jnp.zeros((tm, LANES), jnp.float32)
    lab = jnp.zeros((tm, LANES), jnp.float32)
    vloc = w_refs[0].shape[1]
    for k, w_ref in enumerate(w_refs):
        dist = jnp.broadcast_to(rows[:, lane0 + k:lane0 + k + 1], (tm, LANES)) - lane_f
        for j in range(vloc // NC):
            z = jnp.dot(a, w_ref[:, j * NC:(j + 1) * NC], preferred_element_type=jnp.float32)
            z_ref[:, k * vloc + j * NC:k * vloc + (j + 1) * NC] = z
            cols = [z[:, l * LANES:(l + 1) * LANES] for l in range(NC // LANES)]
            m_new = functools.reduce(jnp.maximum, cols, m)
            s = s * jnp.exp(m - m_new)
            for l, zc in enumerate(cols):
                s = s + jnp.exp(zc - m_new)
                lab = lab + jnp.where(dist == float(j * NC + l * LANES), zc, 0.0)
            m = m_new
    row_m = jnp.max(m, axis=1, keepdims=True)
    row_s = jnp.sum(s * jnp.exp(m - row_m), axis=1, keepdims=True)
    row_l = jnp.sum(lab, axis=1, keepdims=True)
    st_ref[...] = jnp.where(lane == 0, row_m, jnp.where(lane == 1, row_s, row_l)).T[:ROWS]


def logits_call(rows, a_list, w_pair, pair, row_off, n_rows, z_all, hn_all, copy_hn):
    tokens = rows.shape[1]
    d, vloc = w_pair[0].shape
    tiles, off = n_rows // TM1, row_off // TM1
    parts, lo = [], 0
    a_specs = []
    if copy_hn:
        for a in a_list:
            n = a.shape[0] // TM1
            parts.append((lo, lo + n))
            a_specs.append(pl.BlockSpec((TM1, d), lambda i, lo=lo, n=n: (jnp.clip(i - lo, 0, n - 1), 0)))
            lo += n
    else:
        parts.append((0, tiles))
        a_specs.append(pl.BlockSpec((TM1, d), lambda i: (i + off, 0)))
    in_specs = [pl.BlockSpec((ROWS, TM1), lambda i: (0, i + off))] + a_specs
    in_specs += [pl.BlockSpec((d, vloc), lambda i: (0, 0), pipeline_mode=pl.Buffered(1))] * 2
    args = [rows, *a_list, *w_pair]
    out_specs = [pl.BlockSpec((TM1, 2 * vloc), lambda i: (i + off, pair)), pl.BlockSpec((ROWS, TM1), lambda i: (0, i))]
    out_shape = [jax.ShapeDtypeStruct((tokens, 4 * vloc), jnp.float32), jax.ShapeDtypeStruct((ROWS, n_rows), jnp.float32)]
    aliases = {}
    if copy_hn:
        out_specs.append(pl.BlockSpec((TM1, d), lambda i: (i + off, 0)))
        out_shape.append(jax.ShapeDtypeStruct((tokens, d), jnp.bfloat16))
    n_prev = 0
    if z_all is not None:
        aliases[len(args)] = 0
        args.append(z_all)
        n_prev += 1
        if copy_hn:
            aliases[len(args)] = 2
            args.append(hn_all)
            n_prev += 1
    in_specs += [pl.BlockSpec(memory_space=pl.ANY)] * n_prev
    return pl.pallas_call(
        functools.partial(logits_kernel, tuple(parts), 2 * pair, copy_hn, n_prev),
        grid=(tiles,),
        in_specs=in_specs,
        out_specs=out_specs,
        out_shape=out_shape,
        input_output_aliases=aliases,
        compiler_params=pltpu.CompilerParams(dimension_semantics=("arbitrary",), vmem_limit_bytes=56 * 2**20),
        cost_estimate=pl.CostEstimate(
            flops=2 * n_rows * d * 2 * vloc, bytes_accessed=n_rows * 2 * vloc * 4, transcendentals=n_rows * 2 * vloc
        ),
    )(*args)


def grad_kernel(n_prev, rows_ref, z_ref, w0, w1, w2, w3, *refs):
    dz_ref, dhn_ref, w_scr, sem = refs[n_prev:]
    i, blk = pl.program_id(0), pl.program_id(1)

    @pl.when((i == 0) & (blk == 0))
    def _():
        for k, w in enumerate((w0, w1, w2, w3)):
            pltpu.make_async_copy(w, w_scr.at[k], sem.at[k]).start()

    @pl.when(i == 0)
    def _():
        pltpu.make_async_copy(w0, w_scr.at[blk], sem.at[blk]).wait()

    rows = columns_of(rows_ref)
    tm = rows.shape[0]
    lane = lax.broadcasted_iota(jnp.int32, (tm, LANES), 1)
    lab = jnp.sum(jnp.where(lane == blk, rows, 0.0), axis=1, keepdims=True)
    dist = jnp.broadcast_to(lab, (tm, LANES)) - lane.astype(jnp.float32)
    lse = jnp.broadcast_to(rows[:, 4:5], (tm, LANES))
    scale = jnp.broadcast_to(rows[:, 5:6], (tm, LANES))
    vloc = z_ref.shape[1]
    part = None
    for j in range(vloc // NC):
        cols = []
        for l in range(NC // LANES):
            lo = j * NC + l * LANES
            p = jnp.exp(z_ref[:, lo:lo + LANES] - lse)
            p = p - jnp.where(dist == float(lo), 1.0, 0.0)
            cols.append((p * scale).astype(jnp.bfloat16))
        dz = jnp.concatenate(cols, axis=1)
        dz_ref[:, j * NC:(j + 1) * NC] = dz
        prod = lax.dot_general(
            dz, w_scr[blk, :, j * NC:(j + 1) * NC], (((1,), (1,)), ((), ())), preferred_element_type=jnp.float32
        )
        part = prod if part is None else part + prod
    part = part.astype(jnp.bfloat16).astype(jnp.float32)

    @pl.when(blk == 0)
    def _():
        dhn_ref[...] = part

    @pl.when(blk != 0)
    def _():
        dhn_ref[...] += part


def grad_call(rows, z_all, w_list, row_off, n_rows, dz_all):
    tokens = rows.shape[1]
    d, vloc = w_list[0].shape
    tiles, off = n_rows // TM2, row_off // TM2
    any_spec = pl.BlockSpec(memory_space=pl.ANY)
    in_specs = [pl.BlockSpec((ROWS, TM2), lambda i, s: (0, i + off)), pl.BlockSpec((TM2, vloc), lambda i, s: (i + off, s))]
    in_specs += [any_spec] * 4
    args = [rows, z_all, *w_list]
    aliases, n_prev = {}, 0
    if dz_all is not None:
        aliases[len(args)] = 0
        args.append(dz_all)
        in_specs.append(any_spec)
        n_prev = 1
    return pl.pallas_call(
        functools.partial(grad_kernel, n_prev),
        grid=(tiles, 4),
        in_specs=in_specs,
        out_specs=[pl.BlockSpec((TM2, vloc), lambda i, s: (i + off, s)), pl.BlockSpec((TM2, d), lambda i, s: (i, 0))],
        out_shape=[jax.ShapeDtypeStruct((tokens, 4 * vloc), jnp.bfloat16), jax.ShapeDtypeStruct((n_rows, d), jnp.float32)],
        scratch_shapes=[pltpu.VMEM((4, d, vloc), jnp.bfloat16), pltpu.SemaphoreType.DMA((4,))],
        input_output_aliases=aliases,
        compiler_params=pltpu.CompilerParams(dimension_semantics=("arbitrary", "arbitrary"), vmem_limit_bytes=58 * 2**20),
        cost_estimate=pl.CostEstimate(
            flops=2 * n_rows * d * 4 * vloc, bytes_accessed=n_rows * 4 * vloc * 6, transcendentals=n_rows * 4 * vloc
        ),
    )(*args)


def head_kernel(own_ref, core_ref, x_ref, *refs):
    refs[-1][...] = (own_ref[...] + core_ref[...] + x_ref[...]).astype(jnp.bfloat16)


def head_call(own, from_core, from_x, k, prev):
    d, width = from_x.shape
    tile = min(TM1, d)
    wide = pl.BlockSpec((tile, width), lambda i: (i, k))
    args, in_specs, aliases = [own, from_core, from_x], [wide, wide, pl.BlockSpec((tile, width), lambda i: (i, 0))], {}
    if prev is not None:
        args.append(prev)
        in_specs.append(pl.BlockSpec(memory_space=pl.ANY))
        aliases = {3: 0}
    return pl.pallas_call(
        head_kernel,
        grid=(d // tile,),
        in_specs=in_specs,
        out_specs=wide,
        out_shape=jax.ShapeDtypeStruct(own.shape, jnp.bfloat16),
        input_output_aliases=aliases,
        compiler_params=pltpu.CompilerParams(dimension_semantics=("arbitrary",)),
        cost_estimate=pl.CostEstimate(flops=10**6, bytes_accessed=7 * 2**20, transcendentals=0),
    )(*args)


def rows_kernel(base_ref, pair_ref, far_ref, out_ref):
    half = pair_ref.shape[1] // 2
    for pos, (piece, h) in enumerate(ROW_ORDER):
        src = pair_ref if piece < 2 else far_ref
        k = 2 * (piece % 2)
        label = src[k:k + 1, h * half:(h + 1) * half]
        at = slice(pos * half, (pos + 1) * half)
        for q in range(4):
            out_ref[q:q + 1, at] = (label - base_ref[q]).astype(jnp.float32)
        out_ref[4:5, at] = src[k + 1:k + 2, h * half:(h + 1) * half].astype(jnp.float32)
        out_ref[5:, at] = jnp.zeros((ROWS - 5, half), jnp.float32)


def merge_rows(a, b):
    top = jnp.maximum(a[0:1], b[0:1])
    return top, a[1:2] * jnp.exp(a[0:1] - top) + b[1:2] * jnp.exp(b[0:1] - top), a[2:3] + b[2:3]


def local_stats_kernel(a, b, c, d, e, f, out_ref):
    half = a.shape[1] // 2
    first = [(a, 0), (a, 1), (b, 0), (b, 1), (c, 0), (c, 1), (e, 0), (e, 1)]
    second = [(d, k) for k in range(6)] + [(f, 0), (f, 1)]
    for pos, ((x, i), (y, j)) in enumerate(zip(first, second)):
        got = merge_rows(x[:, i * half:(i + 1) * half], y[:, j * half:(j + 1) * half])
        at = slice(pos * half, (pos + 1) * half)
        for k, v in enumerate(got):
            out_ref[k:k + 1, at] = v
        out_ref[3:, at] = jnp.zeros((ROWS - 3, half), jnp.float32)


def peer_stats_kernel(order, mine_ref, theirs_ref, out_ref):
    half = mine_ref.shape[1] // 8
    for pos, src in enumerate(order):
        at = slice(pos * half, (pos + 1) * half)
        got = merge_rows(mine_ref[:, at], theirs_ref[:, src * half:(src + 1) * half])
        for k, v in enumerate(got):
            out_ref[k:k + 1, at] = v
        out_ref[3:, at] = jnp.zeros((ROWS - 3, half), jnp.float32)


def last_stats_kernel(order, kept_ref, rows_ref, mine_ref, theirs_ref, out_ref):
    half = mine_ref.shape[1] // 8
    out_ref[...] = rows_ref[...]
    for pos, src in enumerate(order):
        at = slice(pos * half, (pos + 1) * half)
        top, total, label = merge_rows(mine_ref[:, at], theirs_ref[:, src * half:(src + 1) * half])
        out_ref[4:5, at] = top + jnp.log(total)
        out_ref[5:6, at] = rows_ref[4:5, at] / kept_ref[0]
        out_ref[6:7, at] = label


def small_call(kernel, *args, smem=0):
    width = max(a.shape[-1] for a in args[smem:])
    if kernel is local_stats_kernel or kernel is rows_kernel:
        width = 4 * args[1].shape[1]
    spaces = [pltpu.SMEM] * smem + [pltpu.VMEM] * (len(args) - smem)
    return pl.pallas_call(
        kernel,
        in_specs=[pl.BlockSpec(memory_space=m) for m in spaces],
        out_specs=pl.BlockSpec(memory_space=pltpu.VMEM),
        out_shape=jax.ShapeDtypeStruct((ROWS, width), jnp.float32),
        cost_estimate=pl.CostEstimate(flops=10**6, bytes_accessed=10**6, transcendentals=0),
    )(*args)


ROW_ORDER = ((0, 0), (0, 1), (1, 0), (2, 0), (1, 1), (2, 1), (3, 0), (3, 1))
FROM_Y = tuple(ROW_ORDER.index((p ^ 1, h)) for p, h in ROW_ORDER)
FROM_Z = tuple(ROW_ORDER.index((p ^ 2, h)) for p, h in ROW_ORDER)

CHUNKS = 4


def solution(mesh):
    n_dev = mesh.shape['tp']

    def swap(value, bit):
        return lax.ppermute(value, 'tp', [(i, i ^ bit) for i in range(n_dev)])

    def device_step(hidden, labels, loss_mask, norm_gain, w_head):
        batch, seq, d = hidden.shape
        vloc = w_head.shape[1]
        n_tok = batch * seq
        half = n_tok // 2
        me = lax.axis_index('tp')

        own = jnp.stack([labels.reshape(n_tok), loss_mask.reshape(n_tok)])
        near = jnp.concatenate([own, swap(own, Y)])
        far = swap(near, Z)
        base = jnp.stack([(me ^ q) * vloc for q in range(4)])
        rows1 = small_call(rows_kernel, base, near, far, smem=1)
        kept = jnp.sum((near[1::2] + far[1::2]).astype(jnp.float32)).reshape(1)
        kept = kept + swap(kept, CORE)
        kept = kept + swap(kept, X)

        w_core = swap(w_head, CORE)
        w_x = swap(w_head, X)
        x_rows = hidden.reshape(n_tok, d).astype(jnp.float32)
        hn0, hn1 = (rms_norm(x_rows[i:i + half], norm_gain).astype(jnp.bfloat16) for i in (0, half))
        y0, z0 = swap(hn0, Y), swap(hn0, Z)
        y1, z1 = swap(hn1, Y), swap(hn1, Z)
        d0, d1 = swap(z0, Y), swap(y1, Z)
        w_xc = swap(w_x, CORE)
        w_list = (w_head, w_core, w_x, w_xc)

        def logits(a_list, pair, index, count, z_all, hn_all):
            return logits_call(
                rows1, a_list or [hn_all], w_list[2 * pair:2 * pair + 2], pair, index * half, count * half,
                z_all, hn_all, bool(a_list),
            )

        z_all, st_a, hn_all = logits([hn0, hn1], 0, 0, 2, None, None)
        z_all, st_b, hn_all = logits([y0, z0], 0, 2, 2, z_all, hn_all)
        z_all, st_c, hn_all = logits([y1, z1], 0, 4, 2, z_all, hn_all)
        z_all, st_d = logits(None, 1, 0, 6, z_all, hn_all)
        z_all, st_e, hn_all = logits([d0, d1], 0, 6, 2, z_all, hn_all)
        z_all, st_f = logits(None, 1, 6, 2, z_all, hn_all)

        stats = small_call(local_stats_kernel, st_a, st_b, st_c, st_d, st_e, st_f)
        stats = small_call(functools.partial(peer_stats_kernel, FROM_Y), stats, swap(stats, Y))
        rows2 = small_call(functools.partial(last_stats_kernel, FROM_Z), kept, rows1, stats, swap(stats, Z), smem=1)
        loss_sum = jnp.sum(rows1[4, :n_tok] * (rows2[4, :n_tok] - rows2[6, :n_tok]))

        def grad(index, count, dz_all):
            return grad_call(rows2, z_all, w_list, index * half, count * half, dz_all)

        dz_all, g_d0 = grad(6, 1, None)
        got_z0 = swap(g_d0, Y)
        dz_all, g_d1 = grad(7, 1, dz_all)
        got_y1 = swap(g_d1, Z)
        dz_all, g_y0 = grad(2, 1, dz_all)
        own_y0 = swap(g_y0, Y)
        dz_all, g_z1 = grad(5, 1, dz_all)
        own_z1 = swap(g_z1, Z)
        dz_all, g_z0 = grad(3, 1, dz_all)
        own_z0 = swap(g_z0 + got_z0, Z)
        dz_all, g_y1 = grad(4, 1, dz_all)
        own_y1 = swap(g_y1 + got_y1, Y)
        dz_all, g_own = grad(0, 2, dz_all)

        def head_part(q, lo, size):
            dz = dz_all[:, q * vloc + lo:q * vloc + lo + size]
            return lax.dot_general(hn_all, dz, (((0,), (0,)), ((), ())), preferred_element_type=jnp.float32)

        vc = vloc // CHUNKS
        got_x = []
        for k in range(CHUNKS):
            from_core = swap(head_part(3, k * vc, vc), CORE)
            got_x.append(swap(head_part(2, k * vc, vc) + from_core, X))
        got_c = swap(head_part(1, 0, vloc), CORE)
        d_own = lax.optimization_barrier(head_part(0, 0, vloc))
        d_head = None
        for k in range(CHUNKS):
            d_head = head_call(d_own, got_c, got_x[k], k, d_head)

        d_norm = jnp.concatenate([g_own[:half] + own_y0 + own_z0, g_own[half:] + own_y1 + own_z1])
        _, norm_vjp = jax.vjp(rms_norm, x_rows, norm_gain)
        d_x, d_gain = norm_vjp(d_norm)
        sums = jnp.concatenate([d_gain, jnp.broadcast_to(loss_sum, (LANES,))])
        for bit in (CORE, Y, Z, X):
            sums = sums + swap(sums, bit)
        mean_loss = sums[d] / kept[0]
        return mean_loss, d_x.astype(jnp.bfloat16).reshape(batch, seq, d), d_head, sums[:d]

    return jax.shard_map(device_step, mesh=mesh, in_specs=(P(None, 'tp', None), P(None, 'tp'), P(None, 'tp'), P(), P(None, 'tp')), out_specs=(P(), P(None, 'tp', None), P(None, 'tp'), P()), check_vma=False)
```
